512 devices in a mesh: prow: 16 (over z, core), pcol: 32 (over y, x).
Axes of the slice: x: 4, y: 8, z: 8, core: 2. Of those that a mesh axis runs over, the one named last changes fastest.
Arguments:
- tiles: bfloat16 [16, 32, 32, 256, 256], P('prow', 'pcol')
- tile_brow: int32 [16, 32, 32], P('prow', 'pcol'), may hold values from 0 to 31, as said below
- tile_bcol: int32 [16, 32, 32], P('prow', 'pcol'), may hold values from 0 to 15, as said below
- tile_count: int32 [16, 32], P('prow', 'pcol'), may hold values from 8 to 32, as said below
Outputs:
- row_scale: float32 [32, 16, 256], P(None, 'prow')
- col_scale: float32 [16, 32, 256], P(None, 'pcol')
The draws below stay inside these ranges and needn't reach their ends.
Inputs may be any that keep to these rules, and one draw needn't show every extreme that they name: `tile_brow`: on one device, no two slots name the same pair of local block row and column; the diagonal tile of every block row is present and live, in the first slots of the device that holds it. `tile_bcol`: see tile_brow. `tile_count`: a device that holds diagonal tiles has all 32 slots live, every other device at most 16.
All inputs are finite; a program needn't handle non-finite values.
Results may differ from the reference program's by a relative error of at most 0.0003.
Values sent between devices are 32-bit elements; how exact they have to be, the bound alone decides.
No kernel may reach another device: no remote copies, remote signals or barrier semaphores. Data moves between devices by JAX's collectives and lax.ppermute only.
A program may use at most 64 MiB of HBM per device.

```python
import jax
import jax.numpy as jnp
from jax import lax

TILE = 256
BR_DEV = 32
TILES_DEV = 32
SWEEPS = 3
BC_DEV = 16
N_PROW = 16
N_PCOL = 32


def draw_tiles(key, part):
    shape = (N_PROW, N_PCOL, TILES_DEV, TILE, TILE)
    base = jax.random.normal(jax.random.fold_in(key, 11), shape, jnp.float32)
    span = 2.3
    row_log = jax.random.uniform(jax.random.fold_in(key, 12), (N_PROW, N_PCOL, TILES_DEV, TILE, 1), jnp.float32, -span, span)
    col_log = jax.random.uniform(jax.random.fold_in(key, 13), (N_PROW, N_PCOL, TILES_DEV, 1, TILE), jnp.float32, -span, span)
    return (base * jnp.exp(row_log) * jnp.exp(col_log)).astype(jnp.bfloat16)


def place_slots(key):
    cells = BR_DEV * BC_DEV
    keys = jax.random.split(jax.random.fold_in(key, 21), N_PROW * N_PCOL)
    cell_ids = jnp.arange(cells, dtype=jnp.int32)
    rows_of = cell_ids // BC_DEV
    cols_of = cell_ids % BC_DEV

    def one_device(device_key, position):
        prow_id = position // N_PCOL
        pcol_id = position % N_PCOL
        diagonal = rows_of * N_PROW + prow_id == cols_of * N_PCOL + pcol_id
        order = jax.random.permutation(device_key, cells).astype(jnp.int32)
        score = jnp.where(diagonal, order - cells, order)
        chosen = jnp.argsort(score, stable=True)[:TILES_DEV].astype(jnp.int32)
        return (rows_of[chosen], cols_of[chosen])
    brows, bcols = jax.vmap(one_device)(keys, jnp.arange(N_PROW * N_PCOL, dtype=jnp.int32))
    return (brows.reshape(N_PROW, N_PCOL, TILES_DEV), bcols.reshape(N_PROW, N_PCOL, TILES_DEV))


def draw_tile_brow(key, part):
    return place_slots(key)[0].astype(jnp.int32)


def draw_tile_bcol(key, part):
    return place_slots(key)[1].astype(jnp.int32)


def draw_tile_count(key, part):
    low = max(TILES_DEV // 4, 1)
    high = max(TILES_DEV // 2, low)
    counts = jax.random.randint(jax.random.fold_in(key, 31), (N_PROW, N_PCOL), low, high + 1)
    prow_ids = jnp.arange(N_PROW, dtype=jnp.int32)[:, None]
    pcol_ids = jnp.arange(N_PCOL, dtype=jnp.int32)[None, :]
    holder = pcol_ids % N_PROW == prow_ids
    return jnp.where(holder, TILES_DEV, counts).astype(jnp.int32)


def setup_inputs(seed: int = 0) -> dict:
    key_list = jax.random.split(jax.random.key(seed), 5)
    return {
        "tiles": draw_tiles(jax.random.fold_in(key_list[4], 71), 0),
        "tile_brow": draw_tile_brow(jax.random.fold_in(key_list[4], 71), 0),
        "tile_bcol": draw_tile_bcol(jax.random.fold_in(key_list[4], 71), 0),
        "tile_count": draw_tile_count(jax.random.fold_in(key_list[4], 71), 0),
    }


def rescale(scale, largest):
    return scale / jnp.sqrt(largest)

def reference(tiles, tile_brow, tile_bcol, tile_count):
    live = (jnp.arange(TILES_DEV, dtype=jnp.int32)[None, None, :] < tile_count[:, :, None]).astype(jnp.float32)
    row_vec = jnp.ones((N_PROW, BR_DEV, TILE), jnp.float32)
    col_vec = jnp.ones((N_PCOL, BC_DEV, TILE), jnp.float32)
    col_ids = jnp.arange(N_PCOL, dtype=jnp.int32)[:, None]
    for sweep in range(SWEEPS):

        def one_row(inputs):
            block, brow, bcol, alive, rows = inputs
            row_take = rows[brow]
            col_take = col_vec[col_ids, bcol]
            scaled = jnp.abs(block.astype(jnp.float32)) * row_take[:, :, :, None] * col_take[:, :, None, :]
            row_part = lax.optimization_barrier(jnp.max(scaled, axis=3)) * alive[:, :, None]
            col_part = lax.optimization_barrier(jnp.max(scaled, axis=2)) * alive[:, :, None]
            row_new = jnp.zeros((BR_DEV, TILE), jnp.float32).at[brow.reshape(-1)].max(row_part.reshape(-1, TILE))
            col_new = jnp.zeros((N_PCOL, BC_DEV, TILE), jnp.float32).at[jnp.broadcast_to(col_ids, bcol.shape).reshape(-1), bcol.reshape(-1)].max(col_part.reshape(-1, TILE))
            return (row_new, col_new)
        row_max, col_parts = lax.map(one_row, (tiles, tile_brow, tile_bcol, live, row_vec))
        col_max = lax.optimization_barrier(jnp.max(col_parts, axis=0))
        row_vec = rescale(row_vec, row_max)
        col_vec = rescale(col_vec, col_max)
    return (jnp.transpose(row_vec, (1, 0, 2)), jnp.transpose(col_vec, (1, 0, 2)))
```

```python
import functools

import jax
import jax.numpy as jnp
from jax import lax
from jax.experimental import pallas as pl
from jax.experimental.pallas import tpu as pltpu
from jax.sharding import Mesh
from jax.sharding import PartitionSpec as P

BR_DEV = 32
SWEEPS = 3
PER_COPY = 2
ROWS = 64


def sweep_body(weighted, count, brow, bcol, tiles, *refs):
    if weighted:
        row_scale, col_scale, row_out, col_out, held, turned, sems = refs
    else:
        row_out, col_out, held, sems = refs
    slots, width, _ = held.shape
    copies = slots // PER_COPY

    def fetch(k):
        part = pl.ds(k * PER_COPY, PER_COPY)
        return pltpu.make_async_copy(tiles.at[part], held.at[part], sems.at[k])

    for k in range(copies):
        fetch(k).start()
    row_out[...] = jnp.zeros(row_out.shape, jnp.float32)
    col_out[...] = jnp.zeros(col_out.shape, jnp.float32)
    if weighted:
        pad = jnp.zeros((128 - BR_DEV, width), jnp.float32)
        turned[...] = jnp.concatenate([row_scale[...], pad], axis=0).T
    lanes = lax.broadcasted_iota(jnp.int32, (ROWS, 128), 1)
    rows = lax.broadcasted_iota(jnp.int32, (ROWS, 128), 0)

    def one_tile(s):
        b = brow[s]
        c = bcol[s]
        col_max = None
        row_max = []
        if weighted:
            weight = col_scale[pl.ds(c, 1), :]
            here = lanes == b
        for h in range(0, width, ROWS):
            block = jnp.abs(held[s, pl.ds(h, ROWS), :])
            if weighted:
                own = turned[pl.ds(h, ROWS), :]
                scale = jnp.max(jnp.where(here, own, 0.0), axis=1, keepdims=True)
                block = block.astype(jnp.float32) * scale
                down = jnp.max(block.reshape(ROWS // 8, 8, width), axis=0)
                block = block * weight
                half = jnp.maximum(block[:, :128], block[:, 128:])
            else:
                down = jnp.max(block.reshape(ROWS // 16, 16, width), axis=0)
                half = jnp.maximum(block[:, :128], block[:, 128:]).astype(jnp.float32)
            col_max = down if col_max is None else jnp.maximum(col_max, down)
            across = jnp.max(half, axis=1, keepdims=True)
            placed = jnp.where(lanes == rows + h % 128, across, 0.0)
            placed = jnp.max(placed.reshape(ROWS // 8, 8, 128), axis=0)
            if h % 128:
                row_max[-1] = jnp.maximum(row_max[-1], placed)
            else:
                row_max.append(placed)
        live = s < count[0]
        col_max = jnp.max(col_max.astype(jnp.float32), axis=0, keepdims=True)
        row_max = jnp.concatenate([jnp.max(m, axis=0, keepdims=True) for m in row_max], axis=1)
        col_max = jnp.where(live, col_max, 0.0)
        row_max = jnp.where(live, row_max, 0.0)
        col_out[pl.ds(c, 1), :] = jnp.maximum(col_out[pl.ds(c, 1), :], col_max)
        row_out[pl.ds(b, 1), :] = jnp.maximum(row_out[pl.ds(b, 1), :], row_max)

    def step(k, carry):
        fetch(k).wait()

        @pl.when(k * PER_COPY < count[0])
        def _():
            for t in range(PER_COPY):
                one_tile(k * PER_COPY + t)

        return carry

    lax.fori_loop(0, copies, step, 0)


def sweep_call(tiles, brow, bcol, count, col_blocks, scales=None):
    slots, width, _ = tiles.shape
    smem = pl.BlockSpec(memory_space=pltpu.SMEM)
    vmem = pl.BlockSpec(memory_space=pltpu.VMEM)
    weighted = scales is not None
    scratch = [pltpu.VMEM((slots, width, width), tiles.dtype)]
    if weighted:
        scratch.append(pltpu.VMEM((width, 128), jnp.float32))
    scratch.append(pltpu.SemaphoreType.DMA((slots // PER_COPY,)))
    return pl.pallas_call(
        functools.partial(sweep_body, weighted),
        in_specs=[smem, smem, smem, pl.BlockSpec(memory_space=pltpu.HBM)] + [vmem] * (2 * weighted),
        out_specs=[vmem, vmem],
        out_shape=[
            jax.ShapeDtypeStruct((BR_DEV, width), jnp.float32),
            jax.ShapeDtypeStruct((col_blocks, width), jnp.float32),
        ],
        scratch_shapes=scratch,
        compiler_params=pltpu.CompilerParams(vmem_limit_bytes=16 * 2**20),
        name="weighted_sweep" if weighted else "first_sweep",
    )(count, brow, bcol, tiles, *(scales if weighted else ()))


PROW = ("z", "core")
PCOL = ("y4", "y2", "y1", "x2", "x1")


def from_everyone(value, axes):
    devices = lax.axis_size(axes)
    return lax.all_to_all(
        jnp.broadcast_to(value[None], (devices, *value.shape)), axes, 0, 0, tiled=True
    )


def with_partner(value, axis):
    both = lax.all_gather(value, axis, axis=0)
    return jnp.maximum(both[0], both[1])


def rescale(scale, largest):
    return scale / jnp.sqrt(largest)


def on_device(tiles, tile_brow, tile_bcol, tile_count):
    slots = tiles.shape[2]
    width = tiles.shape[3]
    col_blocks = BR_DEV * lax.axis_size(PROW) // lax.axis_size(PCOL)
    brow = tile_brow.reshape(slots)
    bcol = tile_bcol.reshape(slots)
    count = tile_count.reshape(1)
    block = tiles.reshape(slots, width, width)
    row_vec = col_vec = None
    for sweep in range(SWEEPS):
        scales = (row_vec, col_vec) if sweep else None
        row_max, col_max = sweep_call(block, brow, bcol, count, col_blocks, scales)
        col_max = with_partner(col_max, "core")
        col_max = from_everyone(col_max, "z")
        row_max = with_partner(row_max, "x1")
        row_max = with_partner(row_max, "y1")
        row_max = jnp.max(from_everyone(row_max, ("y4", "y2", "x2")), axis=0)
        col_max = jnp.max(col_max, axis=0)
        if sweep:
            row_vec = rescale(row_vec, row_max)
            col_vec = rescale(col_vec, col_vec * col_max)
        else:
            row_vec = 1.0 / jnp.sqrt(row_max)
            col_vec = 1.0 / jnp.sqrt(col_max)
    return (row_vec.reshape(BR_DEV, 1, width), col_vec.reshape(col_blocks, 1, width))


def solution(mesh):
    shape = (mesh.shape["prow"] // 2, 2, 2, 2, 2, 2, 2)
    finer = Mesh(mesh.devices.reshape(shape), PROW + PCOL)
    in_specs = (
        P(PROW, PCOL, None, None, None),
        P(PROW, PCOL, None),
        P(PROW, PCOL, None),
        P(PROW, PCOL),
    )
    out_specs = (P(None, PROW, None), P(None, PCOL, None))
    return jax.shard_map(
        on_device, mesh=finer, in_specs=in_specs, out_specs=out_specs, check_vma=False
    )
```

```python
import functools

import jax
import jax.numpy as jnp
from jax import lax
from jax.experimental import pallas as pl
from jax.experimental.pallas import tpu as pltpu
from jax.sharding import Mesh
from jax.sharding import PartitionSpec as P

BR_DEV = 32
SWEEPS = 3
PER_COPY = 2
ROWS = 64
LANES = 128
VMEM = 52 * 2**20


def sweep_body(weighted, count_in, brow_in, bcol_in, tiles, *refs):
    if weighted:
        row_scale, col_scale, *refs = refs
    row_out, col_out, count, brow, bcol, held, sems, folded_a, folded_b, *refs = refs
    folded = (folded_a, folded_b)
    if weighted:
        spread, *turned = refs
    slots, width, _ = held.shape
    copies = slots // PER_COPY

    def fetch(k):
        part = pl.ds(k * PER_COPY, PER_COPY)
        return pltpu.make_async_copy(tiles.at[part], held.at[part], sems.at[k])

    small = [
        pltpu.make_async_copy(src, dst, sems.at[copies + i])
        for i, (src, dst) in enumerate(((count_in, count), (brow_in, brow), (bcol_in, bcol)))
    ]
    for copy in small:
        copy.start()
    for k in range(copies):
        fetch(k).start()
    row_out[...] = jnp.zeros(row_out.shape, jnp.float32)
    col_out[...] = jnp.zeros(col_out.shape, jnp.float32)
    if weighted:
        left = row_scale[...]
        parts = []
        for _ in range(3):
            parts.append(left.astype(jnp.bfloat16).astype(jnp.float32))
            left = left - parts[-1]
        parts.append(jnp.zeros((LANES - 3 * BR_DEV, width), jnp.float32))
        spread[...] = jnp.concatenate(parts, axis=0).T.astype(jnp.bfloat16)
    lane = lax.broadcasted_iota(jnp.int32, (ROWS, LANES), 1)
    row = lax.broadcasted_iota(jnp.int32, (ROWS, LANES), 0)
    for copy in small:
        copy.wait()
    live_slots = count[0, 0]

    def turn(s, out):
        part = lax.broadcasted_iota(jnp.int32, (LANES, LANES), 0)
        pick = (part % BR_DEV == brow[0, 0, s]) & (part < 3 * BR_DEV)
        pick = jnp.where(pick, 1.0, 0.0).astype(jnp.bfloat16)
        out[...] = jnp.dot(spread[...], pick, preferred_element_type=jnp.float32)

    def fold(s, scale, out):
        c = bcol[0, 0, s]
        if weighted:
            weight = col_scale[pl.ds(c, 1), :]
        tops = [None, None]
        for h in range(0, width, ROWS):
            block = jnp.abs(held[s, pl.ds(h, ROWS), :])
            best = None
            for side in range(2):
                x = block[:, side * LANES : (side + 1) * LANES]
                group = 16
                if weighted:
                    x = x.astype(jnp.float32) * scale[pl.ds(h, ROWS), :]
                    group = 8
                down = jnp.max(x.reshape(ROWS // group, group, LANES), axis=0)
                tops[side] = down if tops[side] is None else jnp.maximum(tops[side], down)
                if weighted:
                    x = x * weight[:, side * LANES : (side + 1) * LANES]
                best = x if best is None else jnp.maximum(best, x)
            out[pl.ds(h, ROWS), :] = best.astype(jnp.float32)
        top = jnp.concatenate(
            [jnp.max(t.astype(jnp.float32), axis=0, keepdims=True) for t in tops], axis=1
        )
        top = jnp.where(s < live_slots, top, 0.0)
        col_out[pl.ds(c, 1), :] = jnp.maximum(col_out[pl.ds(c, 1), :], top)

    def gather(s, source):
        b = brow[0, 0, jnp.maximum(s, 0)]
        sides = []
        for h in range(0, width, ROWS):
            across = jnp.max(source[pl.ds(h, ROWS), :], axis=1, keepdims=True)
            placed = jnp.where(lane == row + h % LANES, across, 0.0)
            placed = jnp.max(placed.reshape(ROWS // 8, 8, LANES), axis=0)
            if h % LANES:
                sides[-1] = jnp.maximum(sides[-1], placed)
            else:
                sides.append(placed)
        best = jnp.concatenate([jnp.max(p, axis=0, keepdims=True) for p in sides], axis=1)
        best = jnp.where((s >= 0) & (s < live_slots), best, 0.0)
        row_out[pl.ds(b, 1), :] = jnp.maximum(row_out[pl.ds(b, 1), :], best)

    if weighted:
        for t in range(PER_COPY):
            turn(t, turned[0].at[t])

    def step(k, carry):
        for odd in range(2):
            fetch(2 * k + odd).wait()
        for odd in range(2):
            for t in range(PER_COPY):
                s = (2 * k + odd) * PER_COPY + t
                if weighted:
                    turn(jnp.minimum(s + PER_COPY, slots - 1), turned[1 - odd].at[t])
                fold(s, turned[odd].at[t] if weighted else None, folded[odd].at[t])
                gather(s - PER_COPY, folded[1 - odd].at[t])
        return carry

    steps = (live_slots + 2 * PER_COPY - 1) // (2 * PER_COPY)
    lax.fori_loop(0, steps, step, 0)
    for t in range(PER_COPY):
        gather(steps * 2 * PER_COPY - PER_COPY + t, folded[1].at[t])

    def rest(k, carry):
        fetch(k).wait()
        return carry

    lax.fori_loop(2 * steps, copies, rest, 0)


def sweep_call(tiles, brow, bcol, count, col_blocks, scales=None):
    slots, width, _ = tiles.shape
    hbm = pl.BlockSpec(memory_space=pltpu.HBM)
    vmem = pl.BlockSpec(memory_space=pltpu.VMEM)
    weighted = scales is not None
    pair = pltpu.VMEM((PER_COPY, width, LANES), jnp.float32)
    scratch = [pltpu.SMEM(x.shape, x.dtype) for x in (count, brow, bcol)]
    scratch.append(pltpu.VMEM((slots, width, width), tiles.dtype))
    scratch.append(pltpu.SemaphoreType.DMA((slots // PER_COPY + 3,)))
    scratch += [pair, pair]
    if weighted:
        scratch += [pltpu.VMEM((width, LANES), jnp.bfloat16), pair, pair]
    return pl.pallas_call(
        functools.partial(sweep_body, weighted),
        in_specs=[hbm] * 4 + [vmem] * (2 * weighted),
        out_specs=[vmem, vmem],
        out_shape=[
            jax.ShapeDtypeStruct((BR_DEV, width), jnp.float32),
            jax.ShapeDtypeStruct((col_blocks, width), jnp.float32),
        ],
        scratch_shapes=scratch,
        compiler_params=pltpu.CompilerParams(vmem_limit_bytes=VMEM),
        name="weighted_sweep" if weighted else "first_sweep",
    )(count, brow, bcol, tiles, *(scales if weighted else ()))


PROW = ("z", "core")
PCOL = ("y4", "y2", "y1", "x2", "x1")


def from_everyone(value, axes):
    devices = lax.axis_size(axes)
    return lax.all_to_all(
        jnp.broadcast_to(value[None], (devices, *value.shape)), axes, 0, 0, tiled=True
    )


def with_partner(value, axis):
    both = lax.all_gather(value, axis, axis=0)
    return jnp.maximum(both[0], both[1])


def rescale(scale, largest):
    return scale / jnp.sqrt(largest)


def on_device(tiles, tile_brow, tile_bcol, tile_count):
    slots = tiles.shape[2]
    width = tiles.shape[3]
    col_blocks = BR_DEV * lax.axis_size(PROW) // lax.axis_size(PCOL)
    block = tiles.reshape(slots, width, width)
    row_vec = col_vec = None
    for sweep in range(SWEEPS):
        scales = (row_vec, col_vec) if sweep else None
        row_max, col_max = sweep_call(block, tile_brow, tile_bcol, tile_count, col_blocks, scales)
        row_max = jnp.max(from_everyone(row_max, ("x2", "x1", "y1",)), axis=0)
        row_max, col_max = lax.optimization_barrier((row_max, col_max))
        col_max = from_everyone(col_max, PROW)
        row_max = with_partner(row_max, "y4")
        row_max = with_partner(row_max, "y2")
        row_max, col_max = lax.optimization_barrier((row_max, col_max))
        col_max = jnp.max(col_max, axis=0)
        if sweep:
            row_vec = rescale(row_vec, row_max)
            col_vec = rescale(col_vec, col_vec * col_max)
        else:
            row_vec = 1.0 / jnp.sqrt(row_max)
            col_vec = 1.0 / jnp.sqrt(col_max)
    return (row_vec.reshape(BR_DEV, 1, width), col_vec.reshape(col_blocks, 1, width))


def solution(mesh):
    shape = (mesh.shape["prow"] // 2, 2, 2, 2, 2, 2, 2)
    finer = Mesh(mesh.devices.reshape(shape), PROW + PCOL)
    in_specs = (
        P(PROW, PCOL, None, None, None),
        P(PROW, PCOL, None),
        P(PROW, PCOL, None),
        P(PROW, PCOL),
    )
    out_specs = (P(None, PROW, None), P(None, PCOL, None))
    return jax.shard_map(
        on_device, mesh=finer, in_specs=in_specs, out_specs=out_specs, check_vma=False
    )
```

```python
import functools

import jax
import jax.numpy as jnp
from jax import lax
from jax.experimental import pallas as pl
from jax.experimental.pallas import tpu as pltpu
from jax.sharding import Mesh
from jax.sharding import PartitionSpec as P

BR_DEV = 32
SWEEPS = 3
PER_COPY = 2
ROWS = 64
KEPT = 12
FOLD1 = jnp.float32
LANES = 128
VMEM = 52 * 2**20


def sweep_body(weighted, meta_in, tiles, *refs):
    if weighted:
        kept, row_scale, col_scale, row_out, col_out, *refs = refs
    else:
        row_out, col_out, kept, *refs = refs
    meta, held, sems, folded_a, folded_b, *refs = refs
    folded = (folded_a, folded_b)
    if weighted:
        spread, *turned = refs
    first = kept.shape[0]
    width = kept.shape[1]
    slots = first + held.shape[0]
    copies = slots // PER_COPY
    own = first // PER_COPY

    def fetch(k, target, base):
        part = pl.ds(k * PER_COPY, PER_COPY)
        to = pl.ds((k - base) * PER_COPY, PER_COPY)
        return pltpu.make_async_copy(tiles.at[part], target.at[to], sems.at[k])

    about = pltpu.make_async_copy(meta_in, meta, sems.at[copies])
    about.start()
    if not weighted:
        for k in range(own):
            fetch(k, kept, 0).start()
        for k in range(own, copies):
            fetch(k, held, own).start()
    row_out[...] = jnp.zeros(row_out.shape, jnp.float32)
    col_out[...] = jnp.zeros(col_out.shape, jnp.float32)
    about.wait()
    live_slots = meta[0, 2 * slots]
    fetched = copies
    if weighted:
        fetched = jnp.where(live_slots > first, copies, own)

        def get(k, carry):
            fetch(k, held, own).start()
            return carry

        lax.fori_loop(own, fetched, get, 0)
        left = row_scale[...]
        parts = []
        for _ in range(3):
            parts.append(left.astype(jnp.bfloat16).astype(jnp.float32))
            left = left - parts[-1]
        parts.append(jnp.zeros((LANES - 3 * BR_DEV, width), jnp.float32))
        spread[...] = jnp.concatenate(parts, axis=0).T.astype(jnp.bfloat16)

    def turn(s, out):
        part = lax.broadcasted_iota(jnp.int32, (LANES, LANES), 0)
        pick = jnp.where(part % BR_DEV == meta[0, s], 1.0, 0.0).astype(jnp.bfloat16)
        out[...] = jnp.dot(spread[...], pick, preferred_element_type=jnp.float32)

    def fold(s, block_of, scale, out):
        c = meta[0, slots + s]
        if weighted:
            weight = col_scale[pl.ds(c, 1), :]
        tops = [None, None]
        for h in range(0, width, ROWS):
            block = jnp.abs(block_of[pl.ds(h, ROWS), :])
            best = None
            for side in range(2):
                x = block[:, side * LANES : (side + 1) * LANES]
                group = 16
                if weighted:
                    x = x.astype(jnp.float32) * scale[pl.ds(h, ROWS), :]
                    group = 8
                down = jnp.max(x.reshape(ROWS // group, group, LANES), axis=0)
                tops[side] = down if tops[side] is None else jnp.maximum(tops[side], down)
                if weighted:
                    x = x * weight[:, side * LANES : (side + 1) * LANES]
                best = x if best is None else jnp.maximum(best, x)
            out[pl.ds(h, ROWS), :] = best.astype(out.dtype)
        top = jnp.concatenate(
            [jnp.max(t.astype(jnp.float32), axis=0, keepdims=True) for t in tops], axis=1
        )
        top = jnp.where(s < live_slots, top, 0.0)
        col_out[pl.ds(c, 1), :] = jnp.maximum(col_out[pl.ds(c, 1), :], top)

    def gather(s, source):
        b = meta[0, jnp.maximum(s, 0)]
        best = jnp.max(source[...].T, axis=0, keepdims=True).astype(jnp.float32)
        best = jnp.where((s >= 0) & (s < live_slots), best, 0.0)
        row_out[pl.ds(b, 1), :] = jnp.maximum(row_out[pl.ds(b, 1), :], best)

    if weighted:
        for t in range(PER_COPY):
            turn(t, turned[0].at[t])

    def steps_from(target, base, wait):
        def step(k, carry):
            for odd in range(2):
                if wait:
                    fetch(2 * k + odd, target, base).wait()
            for odd in range(2):
                for t in range(PER_COPY):
                    s = (2 * k + odd) * PER_COPY + t
                    if weighted:
                        turn(jnp.minimum(s + PER_COPY, slots - 1), turned[1 - odd].at[t])
                    scale = turned[odd].at[t] if weighted else None
                    fold(s, target.at[s - base * PER_COPY], scale, folded[odd].at[t])
                    gather(s - PER_COPY, folded[1 - odd].at[t])
            return carry

        return step

    steps = (live_slots + 2 * PER_COPY - 1) // (2 * PER_COPY)
    half = own // 2
    lax.fori_loop(0, jnp.minimum(steps, half), steps_from(kept, 0, not weighted), 0)
    lax.fori_loop(half, steps, steps_from(held, own, True), 0)
    for t in range(PER_COPY):
        gather(steps * 2 * PER_COPY - PER_COPY + t, folded[1].at[t])

    def rest(target, base):
        def wait(k, carry):
            fetch(k, target, base).wait()
            return carry

        return wait

    if not weighted:
        lax.fori_loop(2 * jnp.minimum(steps, half), own, rest(kept, 0), 0)
    lax.fori_loop(2 * jnp.maximum(steps, half), fetched, rest(held, own), 0)


def sweep_call(tiles, meta, col_blocks, kept=None, scales=None):
    slots, width, _ = tiles.shape
    hbm = pl.BlockSpec(memory_space=pltpu.HBM)
    vmem = pl.BlockSpec(memory_space=pltpu.VMEM)
    weighted = kept is not None
    pair = (PER_COPY, width, LANES)
    folded = pltpu.VMEM(pair, jnp.float32 if weighted else FOLD1)
    turned = pltpu.VMEM(pair, jnp.float32)
    scratch = [
        pltpu.SMEM(meta.shape, meta.dtype),
        pltpu.VMEM((slots - KEPT, width, width), tiles.dtype),
        pltpu.SemaphoreType.DMA((slots // PER_COPY + 1,)),
        folded,
        folded,
    ]
    out_shape = [
        jax.ShapeDtypeStruct((BR_DEV, width), jnp.float32),
        jax.ShapeDtypeStruct((col_blocks, width), jnp.float32),
    ]
    if weighted:
        scratch += [pltpu.VMEM((width, LANES), jnp.bfloat16), turned, turned]
    else:
        out_shape.append(jax.ShapeDtypeStruct((KEPT, width, width), tiles.dtype))
    return pl.pallas_call(
        functools.partial(sweep_body, weighted),
        in_specs=[hbm] * 2 + [vmem] * (3 * weighted),
        out_specs=[vmem] * len(out_shape),
        out_shape=out_shape,
        scratch_shapes=scratch,
        compiler_params=pltpu.CompilerParams(vmem_limit_bytes=VMEM),
        name="weighted_sweep" if weighted else "first_sweep",
    )(meta, tiles, *((kept, *scales) if weighted else ()))


PROW = ("z", "core")
PCOL = ("y_pair", "y_side", "x")
Y = ("y_pair", "y_side")
NEAR = ((0, 7), (1, 2), (3, 4), (5, 6))
FAR = ((0, 3), (1, 6), (2, 5), (4, 7))


def from_everyone(value, axes):
    devices = lax.axis_size(axes)
    return lax.all_to_all(
        jnp.broadcast_to(value[None], (devices, *value.shape)), axes, 0, 0, tiled=True
    )


def with_partner(value, pairs):
    both = lax.all_gather(value, Y, axis=0, axis_index_groups=pairs)
    return jnp.maximum(both[0], both[1])


def rescale(scale, largest):
    return scale / jnp.sqrt(largest)


def on_device(tiles, tile_brow, tile_bcol, tile_count):
    slots = tiles.shape[2]
    width = tiles.shape[3]
    col_blocks = BR_DEV * lax.axis_size(PROW) // lax.axis_size(PCOL)
    block = tiles.reshape(slots, width, width)
    meta = jnp.concatenate(
        [
            tile_brow.reshape(1, slots),
            tile_bcol.reshape(1, slots),
            jnp.broadcast_to(tile_count, (1, 2 * slots)),
        ],
        axis=1,
    )
    row_vec = col_vec = None
    for sweep in range(SWEEPS):
        if sweep:
            row_max, col_max = sweep_call(block, meta, col_blocks, kept, (row_vec, col_vec))
        else:
            row_max, col_max, kept = sweep_call(block, meta, col_blocks)
        row_max = jnp.max(from_everyone(row_max, ("y_side", "x")), axis=0)
        row_max, col_max = lax.optimization_barrier((row_max, col_max))
        col_max = from_everyone(col_max, PROW)
        row_max = with_partner(row_max, NEAR)
        row_max = with_partner(row_max, FAR)
        row_max, col_max = lax.optimization_barrier((row_max, col_max))
        col_max = jnp.max(col_max, axis=0)
        if sweep:
            row_vec = rescale(row_vec, row_max)
            col_vec = rescale(col_vec, col_vec * col_max)
        else:
            row_vec = 1.0 / jnp.sqrt(row_max)
            col_vec = 1.0 / jnp.sqrt(col_max)
    return (row_vec.reshape(BR_DEV, 1, width), col_vec.reshape(col_blocks, 1, width))


def solution(mesh):
    shape = (mesh.shape["prow"] // 2, 2, mesh.shape["pcol"] // 8, 2, 4)
    finer = Mesh(mesh.devices.reshape(shape), PROW + PCOL)
    in_specs = (
        P(PROW, PCOL, None, None, None),
        P(PROW, PCOL, None),
        P(PROW, PCOL, None),
        P(PROW, PCOL),
    )
    out_specs = (P(None, PROW, None), P(None, PCOL, None))
    return jax.shard_map(
        on_device, mesh=finer, in_specs=in_specs, out_specs=out_specs, check_vma=False
    )
```

```python
import functools

import jax
import jax.numpy as jnp
from jax import lax
from jax.experimental import pallas as pl
from jax.experimental.pallas import tpu as pltpu
from jax.sharding import Mesh
from jax.sharding import PartitionSpec as P

BR_DEV = 32
SWEEPS = 3
PER_COPY = 2
ROWS = 64
KEPT = 12
PACKED = 16
FOLD1 = jnp.bfloat16
LANES = 128
VMEM = 52 * 2**20


def sweep_body(weighted, meta_in, tiles, *refs):
    if weighted:
        kept, row_scale, col_scale, row_out, col_out, *refs = refs
    else:
        row_out, col_out, kept, *refs = refs
    meta, held, sems, folded_a, folded_b, *refs = refs
    folded = (folded_a, folded_b)
    if weighted:
        spread, *turned = refs
    first = kept.shape[0]
    width = kept.shape[1]
    slots = first + held.shape[0]
    copies = slots // PER_COPY
    own = first // PER_COPY

    def fetch(k, target, base):
        part = pl.ds(k * PER_COPY, PER_COPY)
        to = pl.ds((k - base) * PER_COPY, PER_COPY)
        return pltpu.make_async_copy(tiles.at[part], target.at[to], sems.at[k])

    about = pltpu.make_async_copy(meta_in, meta, sems.at[copies])
    about.start()
    if not weighted:
        for k in range(own):
            fetch(k, kept, 0).start()
    for k in range(own, copies):
        fetch(k, held, own).start()
    row_out[...] = jnp.zeros(row_out.shape, jnp.float32)
    col_out[...] = jnp.zeros(col_out.shape, jnp.float32)
    if weighted:
        left = row_scale[...]
        parts = []
        for _ in range(3):
            parts.append(left.astype(jnp.bfloat16).astype(jnp.float32))
            left = left - parts[-1]
        parts.append(jnp.zeros((LANES - 3 * BR_DEV, width), jnp.float32))
        spread[...] = jnp.concatenate(parts, axis=0).T.astype(jnp.bfloat16)
    about.wait()
    live_slots = meta[0, 2 * slots]

    def turn(s, out):
        part = lax.broadcasted_iota(jnp.int32, (LANES, LANES), 0)
        pick = jnp.where(part % BR_DEV == meta[0, s], 1.0, 0.0).astype(jnp.bfloat16)
        out[...] = jnp.dot(spread[...], pick, preferred_element_type=jnp.float32)

    def fold(s, block_of, scale, out):
        c = meta[0, slots + s]
        if weighted:
            weight = col_scale[pl.ds(c, 1), :]
        tops = [None, None]
        for h in range(0, width, ROWS):
            block = jnp.abs(block_of[pl.ds(h, ROWS), :])
            best = None
            for side in range(2):
                x = block[:, side * LANES : (side + 1) * LANES]
                if weighted:
                    x = x.astype(jnp.float32) * scale[pl.ds(h, ROWS), :]
                down = x
                while down.shape[0] > PACKED:
                    half = down.shape[0] // 2
                    down = jnp.maximum(down[:half], down[half:])
                tops[side] = down if tops[side] is None else jnp.maximum(tops[side], down)
                if weighted:
                    x = x * weight[:, side * LANES : (side + 1) * LANES]
                best = x if best is None else jnp.maximum(best, x)
            out[pl.ds(h, ROWS), :] = best.astype(out.dtype)
        top = jnp.concatenate(
            [jnp.max(t.astype(jnp.float32), axis=0, keepdims=True) for t in tops], axis=1
        )
        top = jnp.where(s < live_slots, top, 0.0)
        col_out[pl.ds(c, 1), :] = jnp.maximum(col_out[pl.ds(c, 1), :], top)

    def gather(s, source):
        b = meta[0, jnp.maximum(s, 0)]
        best = jnp.max(source[...].T, axis=0, keepdims=True).astype(jnp.float32)
        best = jnp.where((s >= 0) & (s < live_slots), best, 0.0)
        row_out[pl.ds(b, 1), :] = jnp.maximum(row_out[pl.ds(b, 1), :], best)

    if weighted:
        for t in range(PER_COPY):
            turn(t, turned[0].at[t])

    def steps_from(target, base, wait):
        def step(k, carry):
            for odd in range(2):
                if wait:
                    fetch(2 * k + odd, target, base).wait()
            for odd in range(2):
                for t in range(PER_COPY):
                    s = (2 * k + odd) * PER_COPY + t
                    if weighted:
                        turn(jnp.minimum(s + PER_COPY, slots - 1), turned[1 - odd].at[t])
                    scale = turned[odd].at[t] if weighted else None
                    fold(s, target.at[s - base * PER_COPY], scale, folded[odd].at[t])
                    gather(s - PER_COPY, folded[1 - odd].at[t])
            return carry

        return step

    steps = (live_slots + 2 * PER_COPY - 1) // (2 * PER_COPY)
    half = own // 2
    lax.fori_loop(0, jnp.minimum(steps, half), steps_from(kept, 0, not weighted), 0)
    lax.fori_loop(half, steps, steps_from(held, own, True), 0)
    for t in range(PER_COPY):
        gather(steps * 2 * PER_COPY - PER_COPY + t, folded[1].at[t])

    def rest(target, base):
        def wait(k, carry):
            fetch(k, target, base).wait()
            return carry

        return wait

    if not weighted:
        lax.fori_loop(2 * jnp.minimum(steps, half), own, rest(kept, 0), 0)
    lax.fori_loop(2 * jnp.maximum(steps, half), copies, rest(held, own), 0)


def sweep_call(tiles, meta, col_blocks, kept=None, scales=None):
    slots, width, _ = tiles.shape
    hbm = pl.BlockSpec(memory_space=pltpu.HBM)
    vmem = pl.BlockSpec(memory_space=pltpu.VMEM)
    weighted = kept is not None
    pair = (PER_COPY, width, LANES)
    folded = pltpu.VMEM(pair, jnp.float32 if weighted else FOLD1)
    turned = pltpu.VMEM(pair, jnp.float32)
    scratch = [
        pltpu.SMEM(meta.shape, meta.dtype),
        pltpu.VMEM((slots - KEPT, width, width), tiles.dtype),
        pltpu.SemaphoreType.DMA((slots // PER_COPY + 1,)),
        folded,
        folded,
    ]
    out_shape = [
        jax.ShapeDtypeStruct((BR_DEV, width), jnp.float32),
        jax.ShapeDtypeStruct((col_blocks, width), jnp.float32),
    ]
    if weighted:
        scratch += [pltpu.VMEM((width, LANES), jnp.bfloat16), turned, turned]
    else:
        out_shape.append(jax.ShapeDtypeStruct((KEPT, width, width), tiles.dtype))
    return pl.pallas_call(
        functools.partial(sweep_body, weighted),
        in_specs=[hbm] * 2 + [vmem] * (3 * weighted),
        out_specs=[vmem] * len(out_shape),
        out_shape=out_shape,
        scratch_shapes=scratch,
        compiler_params=pltpu.CompilerParams(vmem_limit_bytes=VMEM),
        name="weighted_sweep" if weighted else "first_sweep",
    )(meta, tiles, *((kept, *scales) if weighted else ()))


PROW = ("z", "core")
PCOL = ("y_pair", "y_side", "x")
Y = ("y_pair", "y_side")
NEAR = ((0, 7), (1, 2), (3, 4), (5, 6))
FAR = ((0, 3), (1, 6), (2, 5), (4, 7))


def from_everyone(value, axes):
    devices = lax.axis_size(axes)
    return lax.all_to_all(
        jnp.broadcast_to(value[None], (devices, *value.shape)), axes, 0, 0, tiled=True
    )


def with_partner(value, pairs):
    both = lax.all_gather(value, Y, axis=0, axis_index_groups=pairs)
    return jnp.maximum(both[0], both[1])


def rescale(scale, largest):
    return scale / jnp.sqrt(largest)


def on_device(tiles, tile_brow, tile_bcol, tile_count):
    slots = tiles.shape[2]
    width = tiles.shape[3]
    col_blocks = BR_DEV * lax.axis_size(PROW) // lax.axis_size(PCOL)
    block = tiles.reshape(slots, width, width)
    meta = jnp.concatenate(
        [
            tile_brow.reshape(1, slots),
            tile_bcol.reshape(1, slots),
            jnp.broadcast_to(tile_count, (1, 2 * slots)),
        ],
        axis=1,
    )
    row_vec = col_vec = None
    for sweep in range(SWEEPS):
        if sweep:
            row_max, col_max = sweep_call(block, meta, col_blocks, kept, (row_vec, col_vec))
        else:
            row_max, col_max, kept = sweep_call(block, meta, col_blocks)
        row_max = from_everyone(row_max, ("y_side", "x"))
        row_max, col_max = lax.optimization_barrier((row_max, col_max))
        row_max = jnp.max(row_max, axis=0)
        col_max = from_everyone(col_max, PROW)
        row_max = with_partner(row_max, NEAR)
        row_max = with_partner(row_max, FAR)
        row_max, col_max = lax.optimization_barrier((row_max, col_max))
        col_max = jnp.max(col_max, axis=0)
        if sweep:
            row_vec = rescale(row_vec, row_max)
            col_vec = rescale(col_vec, col_vec * col_max)
        else:
            row_vec = 1.0 / jnp.sqrt(row_max)
            col_vec = 1.0 / jnp.sqrt(col_max)
    return (row_vec.reshape(BR_DEV, 1, width), col_vec.reshape(col_blocks, 1, width))


def solution(mesh):
    shape = (mesh.shape["prow"] // 2, 2, mesh.shape["pcol"] // 8, 2, 4)
    finer = Mesh(mesh.devices.reshape(shape), PROW + PCOL)
    in_specs = (
        P(PROW, PCOL, None, None, None),
        P(PROW, PCOL, None),
        P(PROW, PCOL, None),
        P(PROW, PCOL),
    )
    out_specs = (P(None, PROW, None), P(None, PCOL, None))
    return jax.shard_map(
        on_device, mesh=finer, in_specs=in_specs, out_specs=out_specs, check_vma=False
    )
```

```python
import functools

import jax
import jax.numpy as jnp
from jax import lax
from jax.experimental import pallas as pl
from jax.experimental.pallas import tpu as pltpu
from jax.sharding import Mesh
from jax.sharding import PartitionSpec as P

BR_DEV = 32
SWEEPS = 3
PER_COPY = 2
ROWS = 64
KEPT = 12
PACKED = 16
FOLD1 = jnp.bfloat16
LANES = 128
VMEM = 52 * 2**20


def sweep_body(weighted, meta_in, tiles, *refs):
    if weighted:
        kept, row_scale, col_scale, row_out, col_all, *refs = refs
    else:
        row_out, col_all, kept, *refs = refs
    meta, held, sems, col_sems, col_out, folded_a, folded_b, *refs = refs
    folded = (folded_a, folded_b)
    if weighted:
        spread, *turned = refs
    first = kept.shape[0]
    width = kept.shape[1]
    slots = first + held.shape[0]
    copies = slots // PER_COPY
    own = first // PER_COPY

    def fetch(k, target, base):
        part = pl.ds(k * PER_COPY, PER_COPY)
        to = pl.ds((k - base) * PER_COPY, PER_COPY)
        return pltpu.make_async_copy(tiles.at[part], target.at[to], sems.at[k])

    about = pltpu.make_async_copy(meta_in, meta, sems.at[copies])
    about.start()
    if not weighted:
        for k in range(own):
            fetch(k, kept, 0).start()
    for k in range(own, copies):
        fetch(k, held, own).start()
    row_out[...] = jnp.zeros(row_out.shape, jnp.float32)
    col_out[...] = jnp.zeros(col_out.shape, jnp.float32)
    if weighted:
        left = row_scale[...]
        parts = []
        for _ in range(3):
            parts.append(left.astype(jnp.bfloat16).astype(jnp.float32))
            left = left - parts[-1]
        parts.append(jnp.zeros((LANES - 3 * BR_DEV, width), jnp.float32))
        spread[...] = jnp.concatenate(parts, axis=0).T.astype(jnp.bfloat16)
    about.wait()
    live_slots = meta[0, 2 * slots]

    def turn(s, out):
        part = lax.broadcasted_iota(jnp.int32, (LANES, LANES), 0)
        pick = jnp.where(part % BR_DEV == meta[0, s], 1.0, 0.0).astype(jnp.bfloat16)
        out[...] = jnp.dot(spread[...], pick, preferred_element_type=jnp.float32)

    def fold(s, block_of, scale, out):
        c = meta[0, slots + s]
        if weighted:
            weight = col_scale[pl.ds(c, 1), :]
        tops = [None, None]
        for h in range(0, width, ROWS):
            block = jnp.abs(block_of[pl.ds(h, ROWS), :])
            best = None
            for side in range(2):
                x = block[:, side * LANES : (side + 1) * LANES]
                if weighted:
                    x = x.astype(jnp.float32) * scale[pl.ds(h, ROWS), :]
                down = x
                while down.shape[0] > PACKED:
                    half = down.shape[0] // 2
                    down = jnp.maximum(down[:half], down[half:])
                tops[side] = down if tops[side] is None else jnp.maximum(tops[side], down)
                if weighted:
                    x = x * weight[:, side * LANES : (side + 1) * LANES]
                best = x if best is None else jnp.maximum(best, x)
            out[pl.ds(h, ROWS), :] = best.astype(out.dtype)
        top = jnp.concatenate(
            [jnp.max(t.astype(jnp.float32), axis=0, keepdims=True) for t in tops], axis=1
        )
        top = jnp.where(s < live_slots, top, 0.0)
        col_out[pl.ds(c, 1), :] = jnp.maximum(col_out[pl.ds(c, 1), :], top)

    def gather(s, source):
        b = meta[0, jnp.maximum(s, 0)]
        best = jnp.max(source[...].T, axis=0, keepdims=True).astype(jnp.float32)
        best = jnp.where((s >= 0) & (s < live_slots), best, 0.0)
        row_out[pl.ds(b, 1), :] = jnp.maximum(row_out[pl.ds(b, 1), :], best)

    if weighted:
        for t in range(PER_COPY):
            turn(t, turned[0].at[t])

    def steps_from(target, base, wait):
        def step(k, carry):
            for odd in range(2):
                if wait:
                    fetch(2 * k + odd, target, base).wait()
            for odd in range(2):
                for t in range(PER_COPY):
                    s = (2 * k + odd) * PER_COPY + t
                    if weighted:
                        turn(jnp.minimum(s + PER_COPY, slots - 1), turned[1 - odd].at[t])
                    scale = turned[odd].at[t] if weighted else None
                    fold(s, target.at[s - base * PER_COPY], scale, folded[odd].at[t])
                    gather(s - PER_COPY, folded[1 - odd].at[t])
            return carry

        return step

    steps = (live_slots + 2 * PER_COPY - 1) // (2 * PER_COPY)
    half = own // 2
    lax.fori_loop(0, jnp.minimum(steps, half), steps_from(kept, 0, not weighted), 0)
    lax.fori_loop(half, steps, steps_from(held, own, True), 0)
    away = [
        pltpu.make_async_copy(col_out, col_all.at[d], col_sems.at[d])
        for d in range(col_all.shape[0])
    ]
    for copy in away:
        copy.start()
    for t in range(PER_COPY):
        gather(steps * 2 * PER_COPY - PER_COPY + t, folded[1].at[t])
    for copy in away:
        copy.wait()

    def rest(target, base):
        def wait(k, carry):
            fetch(k, target, base).wait()
            return carry

        return wait

    if not weighted:
        lax.fori_loop(2 * jnp.minimum(steps, half), own, rest(kept, 0), 0)
    lax.fori_loop(2 * jnp.maximum(steps, half), copies, rest(held, own), 0)


def sweep_call(tiles, meta, col_blocks, peers, kept=None, scales=None):
    slots, width, _ = tiles.shape
    hbm = pl.BlockSpec(memory_space=pltpu.HBM)
    vmem = pl.BlockSpec(memory_space=pltpu.VMEM)
    weighted = kept is not None
    pair = (PER_COPY, width, LANES)
    folded = pltpu.VMEM(pair, jnp.float32 if weighted else FOLD1)
    turned = pltpu.VMEM(pair, jnp.float32)
    scratch = [
        pltpu.SMEM(meta.shape, meta.dtype),
        pltpu.VMEM((slots - KEPT, width, width), tiles.dtype),
        pltpu.SemaphoreType.DMA((slots // PER_COPY + 1,)),
        pltpu.SemaphoreType.DMA((peers,)),
        pltpu.VMEM((col_blocks, width), jnp.float32),
        folded,
        folded,
    ]
    out_shape = [
        jax.ShapeDtypeStruct((BR_DEV, width), jnp.float32),
        jax.ShapeDtypeStruct((peers, col_blocks, width), jnp.float32),
    ]
    if weighted:
        scratch += [pltpu.VMEM((width, LANES), jnp.bfloat16), turned, turned]
    else:
        out_shape.append(jax.ShapeDtypeStruct((KEPT, width, width), tiles.dtype))
    return pl.pallas_call(
        functools.partial(sweep_body, weighted),
        in_specs=[hbm] * 2 + [vmem] * (3 * weighted),
        out_specs=[vmem, hbm, vmem][: len(out_shape)],
        out_shape=out_shape,
        scratch_shapes=scratch,
        compiler_params=pltpu.CompilerParams(vmem_limit_bytes=VMEM),
        name="weighted_sweep" if weighted else "first_sweep",
    )(meta, tiles, *((kept, *scales) if weighted else ()))


PROW = ("z", "core")
PCOL = ("y_pair", "y_side", "x")
Y = ("y_pair", "y_side")
NEAR = ((0, 7), (1, 2), (3, 4), (5, 6))
FAR = ((0, 3), (1, 6), (2, 5), (4, 7))


def from_everyone(value, axes):
    devices = lax.axis_size(axes)
    return lax.all_to_all(
        jnp.broadcast_to(value[None], (devices, *value.shape)), axes, 0, 0, tiled=True
    )


def with_partner(value, pairs):
    both = lax.all_gather(value, Y, axis=0, axis_index_groups=pairs)
    return jnp.maximum(both[0], both[1])


def rescale(scale, largest):
    return scale / jnp.sqrt(largest)


def on_device(tiles, tile_brow, tile_bcol, tile_count):
    slots = tiles.shape[2]
    width = tiles.shape[3]
    col_blocks = BR_DEV * lax.axis_size(PROW) // lax.axis_size(PCOL)
    block = tiles.reshape(slots, width, width)
    meta = jnp.concatenate(
        [
            tile_brow.reshape(1, slots),
            tile_bcol.reshape(1, slots),
            jnp.broadcast_to(tile_count, (1, 2 * slots)),
        ],
        axis=1,
    )
    peers = lax.axis_size(PROW)
    row_vec = col_vec = None
    for sweep in range(SWEEPS):
        if sweep:
            scales = (row_vec, col_vec)
            row_max, col_max = sweep_call(block, meta, col_blocks, peers, kept, scales)
        else:
            row_max, col_max, kept = sweep_call(block, meta, col_blocks, peers)
        row_max = from_everyone(row_max, ("y_side", "x"))
        row_max, col_max = lax.optimization_barrier((row_max, col_max))
        row_max = jnp.max(row_max, axis=0)
        col_max = lax.all_to_all(col_max, PROW, 0, 0, tiled=True)
        row_max = with_partner(row_max, NEAR)
        row_max = with_partner(row_max, FAR)
        row_max, col_max = lax.optimization_barrier((row_max, col_max))
        col_max = jnp.max(col_max, axis=0)
        if sweep:
            row_vec = rescale(row_vec, row_max)
            col_vec = rescale(col_vec, col_vec * col_max)
        else:
            row_vec = 1.0 / jnp.sqrt(row_max)
            col_vec = 1.0 / jnp.sqrt(col_max)
    return (row_vec.reshape(BR_DEV, 1, width), col_vec.reshape(col_blocks, 1, width))


def solution(mesh):
    shape = (mesh.shape["prow"] // 2, 2, mesh.shape["pcol"] // 8, 2, 4)
    finer = Mesh(mesh.devices.reshape(shape), PROW + PCOL)
    in_specs = (
        P(PROW, PCOL, None, None, None),
        P(PROW, PCOL, None),
        P(PROW, PCOL, None),
        P(PROW, PCOL),
    )
    out_specs = (P(None, PROW, None), P(None, PCOL, None))
    return jax.shard_map(
        on_device, mesh=finer, in_specs=in_specs, out_specs=out_specs, check_vma=False
    )
```

```python
import functools

import jax
import jax.numpy as jnp
from jax import lax
from jax.experimental import pallas as pl
from jax.experimental.pallas import tpu as pltpu
from jax.sharding import Mesh
from jax.sharding import PartitionSpec as P

BR_DEV = 32
SWEEPS = 3
PER_COPY = 2
ROWS = 64
KEPT = 12
PACKED = 16
FOLD1 = jnp.bfloat16
LANES = 128
VMEM = 52 * 2**20


def sweep_body(weighted, meta_in, tiles, *refs):
    if weighted:
        kept, row_scale, col_scale, row_out, col_all, *refs = refs
    else:
        row_out, col_all, kept, *refs = refs
    meta, held, sems, col_sems, col_out, folded_a, folded_b, *refs = refs
    folded = (folded_a, folded_b)
    if weighted:
        spread, *turned = refs
    first = kept.shape[0]
    width = kept.shape[1]
    slots = first + held.shape[0]
    copies = slots // PER_COPY
    own = first // PER_COPY

    def fetch(k, target, base):
        part = pl.ds(k * PER_COPY, PER_COPY)
        to = pl.ds((k - base) * PER_COPY, PER_COPY)
        return pltpu.make_async_copy(tiles.at[part], target.at[to], sems.at[k])

    about = pltpu.make_async_copy(meta_in, meta, sems.at[copies])
    about.start()
    if not weighted:
        for k in range(own):
            fetch(k, kept, 0).start()
    for k in range(own, copies):
        fetch(k, held, own).start()
    row_out[...] = jnp.zeros(row_out.shape, jnp.float32)
    col_out[...] = jnp.zeros(col_out.shape, jnp.float32)
    if weighted:
        left = row_scale[...]
        parts = []
        for _ in range(3):
            parts.append(left.astype(jnp.bfloat16).astype(jnp.float32))
            left = left - parts[-1]
        parts.append(jnp.zeros((LANES - 3 * BR_DEV, width), jnp.float32))
        spread[...] = jnp.concatenate(parts, axis=0).T.astype(jnp.bfloat16)
    about.wait()
    live_slots = meta[0, 2 * slots]

    def turn(s, out):
        part = lax.broadcasted_iota(jnp.int32, (LANES, LANES), 0)
        pick = jnp.where(part % BR_DEV == meta[0, s], 1.0, 0.0).astype(jnp.bfloat16)
        out[...] = jnp.dot(spread[...], pick, preferred_element_type=jnp.float32)

    def fold(s, block_of, scale, out):
        c = meta[0, slots + s]
        if weighted:
            weight = col_scale[pl.ds(c, 1), :]
        tops = [None, None]
        for h in range(0, width, ROWS):
            block = jnp.abs(block_of[pl.ds(h, ROWS), :])
            best = None
            for side in range(2):
                x = block[:, side * LANES : (side + 1) * LANES]
                if weighted:
                    x = x.astype(jnp.float32) * scale[pl.ds(h, ROWS), :]
                down = x
                while down.shape[0] > PACKED:
                    half = down.shape[0] // 2
                    down = jnp.maximum(down[:half], down[half:])
                tops[side] = down if tops[side] is None else jnp.maximum(tops[side], down)
                if weighted:
                    x = x * weight[:, side * LANES : (side + 1) * LANES]
                best = x if best is None else jnp.maximum(best, x)
            out[pl.ds(h, ROWS), :] = best.astype(out.dtype)
        top = jnp.concatenate(
            [jnp.max(t.astype(jnp.float32), axis=0, keepdims=True) for t in tops], axis=1
        )
        top = jnp.where(s < live_slots, top, 0.0)
        col_out[pl.ds(c, 1), :] = jnp.maximum(col_out[pl.ds(c, 1), :], top)

    def gather(s, source):
        b = meta[0, jnp.maximum(s, 0)]
        best = jnp.max(source[...].T, axis=0, keepdims=True).astype(jnp.float32)
        best = jnp.where((s >= 0) & (s < live_slots), best, 0.0)
        row_out[pl.ds(b, 1), :] = jnp.maximum(row_out[pl.ds(b, 1), :], best)

    if weighted:
        for t in range(PER_COPY):
            turn(t, turned[0].at[t])

    def steps_from(target, base, wait):
        def step(k, carry):
            for odd in range(2):
                if wait:
                    fetch(2 * k + odd, target, base).wait()
            for odd in range(2):
                for t in range(PER_COPY):
                    s = (2 * k + odd) * PER_COPY + t
                    if weighted:
                        turn(jnp.minimum(s + PER_COPY, slots - 1), turned[1 - odd].at[t])
                    scale = turned[odd].at[t] if weighted else None
                    fold(s, target.at[s - base * PER_COPY], scale, folded[odd].at[t])
                    gather(s - PER_COPY, folded[1 - odd].at[t])
            return carry

        return step

    steps = (live_slots + 2 * PER_COPY - 1) // (2 * PER_COPY)
    half = own // 2
    lax.fori_loop(0, jnp.minimum(steps, half), steps_from(kept, 0, not weighted), 0)
    lax.fori_loop(half, steps, steps_from(held, own, True), 0)
    away = [
        pltpu.make_async_copy(col_out, col_all.at[d], col_sems.at[d])
        for d in range(col_all.shape[0])
    ]
    for copy in away:
        copy.start()
    for t in range(PER_COPY):
        gather(steps * 2 * PER_COPY - PER_COPY + t, folded[1].at[t])
    for copy in away:
        copy.wait()

    def rest(target, base):
        def wait(k, carry):
            fetch(k, target, base).wait()
            return carry

        return wait

    if not weighted:
        lax.fori_loop(2 * jnp.minimum(steps, half), own, rest(kept, 0), 0)
    lax.fori_loop(2 * jnp.maximum(steps, half), copies, rest(held, own), 0)


def sweep_call(tiles, meta, col_blocks, peers, kept=None, scales=None):
    slots, width, _ = tiles.shape
    hbm = pl.BlockSpec(memory_space=pltpu.HBM)
    vmem = pl.BlockSpec(memory_space=pltpu.VMEM)
    weighted = kept is not None
    pair = (PER_COPY, width, LANES)
    folded = pltpu.VMEM(pair, jnp.float32 if weighted else FOLD1)
    turned = pltpu.VMEM(pair, jnp.float32)
    scratch = [
        pltpu.SMEM(meta.shape, meta.dtype),
        pltpu.VMEM((slots - KEPT, width, width), tiles.dtype),
        pltpu.SemaphoreType.DMA((slots // PER_COPY + 1,)),
        pltpu.SemaphoreType.DMA((peers,)),
        pltpu.VMEM((col_blocks, width), jnp.float32),
        folded,
        folded,
    ]
    out_shape = [
        jax.ShapeDtypeStruct((BR_DEV, width), jnp.float32),
        jax.ShapeDtypeStruct((peers, col_blocks, width), jnp.float32),
    ]
    if weighted:
        scratch += [pltpu.VMEM((width, LANES), jnp.bfloat16), turned, turned]
    else:
        out_shape.append(jax.ShapeDtypeStruct((KEPT, width, width), tiles.dtype))
    return pl.pallas_call(
        functools.partial(sweep_body, weighted),
        in_specs=[hbm] * 2 + [vmem] * (3 * weighted),
        out_specs=[vmem, hbm, vmem][: len(out_shape)],
        out_shape=out_shape,
        scratch_shapes=scratch,
        compiler_params=pltpu.CompilerParams(vmem_limit_bytes=VMEM),
        name="weighted_sweep" if weighted else "first_sweep",
    )(meta, tiles, *((kept, *scales) if weighted else ()))


def last_body(row_scale, col_scale, row_max, col_all, row_out, col_out):
    col_max = jnp.max(col_all[...], axis=0)
    row_out[:, 0, :] = rescale(row_scale[...], row_max[...])
    col_out[:, 0, :] = rescale(col_scale[...], col_scale[...] * col_max)


def last_call(*operands):
    vmem = pl.BlockSpec(memory_space=pltpu.VMEM)
    return pl.pallas_call(
        last_body,
        in_specs=[vmem] * 4,
        out_specs=[vmem] * 2,
        out_shape=[
            jax.ShapeDtypeStruct((x.shape[0], 1, x.shape[1]), jnp.float32) for x in operands[:2]
        ],
        compiler_params=pltpu.CompilerParams(vmem_limit_bytes=VMEM),
        name="last_scales",
    )(*operands)


PROW = ("z", "core")
PCOL = ("y_pair", "y_side", "x")
Y = ("y_pair", "y_side")
NEAR = ((0, 7), (1, 2), (3, 4), (5, 6))
FAR = ((0, 3), (1, 6), (2, 5), (4, 7))


def from_everyone(value, axes):
    devices = lax.axis_size(axes)
    return lax.all_to_all(
        jnp.broadcast_to(value[None], (devices, *value.shape)), axes, 0, 0, tiled=True
    )


def with_partner(value, pairs):
    both = lax.all_gather(value, Y, axis=0, axis_index_groups=pairs)
    return jnp.maximum(both[0], both[1])


def rescale(scale, largest):
    return scale / jnp.sqrt(largest)


def on_device(tiles, tile_brow, tile_bcol, tile_count):
    slots = tiles.shape[2]
    width = tiles.shape[3]
    col_blocks = BR_DEV * lax.axis_size(PROW) // lax.axis_size(PCOL)
    block = tiles.reshape(slots, width, width)
    meta = jnp.concatenate(
        [
            tile_brow.reshape(1, slots),
            tile_bcol.reshape(1, slots),
            jnp.broadcast_to(tile_count, (1, 2 * slots)),
        ],
        axis=1,
    )
    peers = lax.axis_size(PROW)
    row_vec = col_vec = None
    for sweep in range(SWEEPS):
        if sweep:
            scales = (row_vec, col_vec)
            row_max, col_max = sweep_call(block, meta, col_blocks, peers, kept, scales)
        else:
            row_max, col_max, kept = sweep_call(block, meta, col_blocks, peers)
        row_max = from_everyone(row_max, ("x", "y_side"))
        row_max, col_max = lax.optimization_barrier((row_max, col_max))
        row_max = jnp.max(row_max, axis=0)
        col_max = lax.all_to_all(col_max, ("core", "z"), 0, 0, tiled=True)
        row_max = with_partner(row_max, NEAR)
        row_max = with_partner(row_max, FAR)
        row_max, col_max = lax.optimization_barrier((row_max, col_max))
        if sweep == SWEEPS - 1:
            return tuple(last_call(row_vec, col_vec, row_max, col_max))
        col_max = jnp.max(col_max, axis=0)
        if sweep:
            row_vec = rescale(row_vec, row_max)
            col_vec = rescale(col_vec, col_vec * col_max)
        else:
            row_vec = 1.0 / jnp.sqrt(row_max)
            col_vec = 1.0 / jnp.sqrt(col_max)


def solution(mesh):
    shape = (mesh.shape["prow"] // 2, 2, mesh.shape["pcol"] // 8, 2, 4)
    finer = Mesh(mesh.devices.reshape(shape), PROW + PCOL)
    in_specs = (
        P(PROW, PCOL, None, None, None),
        P(PROW, PCOL, None),
        P(PROW, PCOL, None),
        P(PROW, PCOL),
    )
    out_specs = (P(None, PROW, None), P(None, PCOL, None))
    return jax.shard_map(
        on_device, mesh=finer, in_specs=in_specs, out_specs=out_specs, check_vma=False
    )
```
